32 devices in a mesh: dp: 2 (over x), my: 4 (over z), mx: 4 (over y, core).
Axes of the slice: x: 2, y: 2, z: 4, core: 2. Of those that a mesh axis runs over, the one named last changes fastest.
Arguments:
- tokens: bfloat16 [2, 256, 5120], P('dp', None, 'my'), parts along dimension 0
- ln_scale: bfloat16 [5120], P('my')
- w_in: bfloat16 [5120, 35840], P('my', 'mx')
- mlp_bias: bfloat16 [20480], P('mx')
- q_scale: bfloat16 [128], replicated
- k_scale: bfloat16 [128], replicated
- w_out: bfloat16 [25600, 5120], P('mx', 'my')
- attn_out_bias: bfloat16 [5120], P('my')
- mlp_out_bias: bfloat16 [5120], P('my')
Outputs:
- output: bfloat16 [2, 256, 5120], P('dp', None, 'my'), parts along dimension 0
There are 2 independent parts. The reference program is written for one: setup_inputs(seed, part) draws one part's arguments, and reference() takes and returns one part's arrays. A program takes and returns all parts, laid end to end along the dimension named above; an argument that names none is the same for every part.
All inputs are finite; a program needn't handle non-finite values.
Results may differ from the reference program's by a relative error of at most 0.0126557.
Values are sent between devices in bfloat16 or wider.
A program may use at most 1 GiB of HBM per device.

```python
import jax
import jax.numpy as jnp
from jax import lax

BATCH = 1
SEQ = 256
D = 5120
HEADS = 40
HEAD = 128
FF = 20480
BLOCKS = 4

HEADS_BLK = HEADS // BLOCKS
FF_BLK = FF // BLOCKS
QKV_BLK = HEADS_BLK * HEAD
IN_BLK = 3 * QKV_BLK + FF_BLK


def block_columns(pieces):
    per_block = [one_piece.reshape(D, BLOCKS, one_piece.shape[1] // BLOCKS) for one_piece in pieces]
    return jnp.concatenate(per_block, axis=2).reshape(D, -1)


def block_rows(pieces):
    per_block = [one_piece.reshape(BLOCKS, one_piece.shape[0] // BLOCKS, D) for one_piece in pieces]
    return jnp.concatenate(per_block, axis=1).reshape(-1, D)


def setup_inputs(seed: int = 0, part: int = 0) -> dict:
    root_key = jax.random.key(seed)
    shared_keys = jax.random.split(root_key, 12)
    part_keys = jax.random.split(jax.random.fold_in(root_key, part), 4)
    width_grid = jnp.linspace(-1.0, 1.0, D)
    mean_amp = jax.random.uniform(part_keys[0], (), jnp.float32, minval=0.6, maxval=1.2)
    scale_amp = jax.random.uniform(part_keys[1], (), jnp.float32, minval=0.3, maxval=0.6)
    row_offset = 0.3 * jax.random.normal(part_keys[2], (BATCH, SEQ, 1), jnp.float32)
    base_noise = jax.random.normal(part_keys[3], (BATCH, SEQ, D), jnp.float32)
    tokens = base_noise * jnp.exp(scale_amp * width_grid) + mean_amp * width_grid + row_offset
    in_gain = D ** -0.5
    w_query = jax.random.normal(shared_keys[0], (D, HEADS * HEAD), jnp.float32) * in_gain
    w_key = jax.random.normal(shared_keys[1], (D, HEADS * HEAD), jnp.float32) * in_gain
    w_value = jax.random.normal(shared_keys[2], (D, HEADS * HEAD), jnp.float32) * in_gain
    w_up = jax.random.normal(shared_keys[3], (D, FF), jnp.float32) * in_gain
    w_attn_out = jax.random.normal(shared_keys[4], (HEADS * HEAD, D), jnp.float32) * (HEADS * HEAD) ** -0.5
    w_down = jax.random.normal(shared_keys[5], (FF, D), jnp.float32) * FF ** -0.5
    return {
        'tokens': tokens.astype(jnp.bfloat16),
        'ln_scale': jax.random.uniform(shared_keys[6], (D,), jnp.float32, minval=0.5, maxval=1.5).astype(jnp.bfloat16),
        'w_in': block_columns([w_query, w_key, w_value, w_up]).astype(jnp.bfloat16),
        'mlp_bias': (0.5 * jax.random.normal(shared_keys[7], (FF,), jnp.float32)).astype(jnp.bfloat16),
        'q_scale': jax.random.uniform(shared_keys[8], (HEAD,), jnp.float32, minval=1.2, maxval=2.0).astype(jnp.bfloat16),
        'k_scale': jax.random.uniform(shared_keys[9], (HEAD,), jnp.float32, minval=1.2, maxval=2.0).astype(jnp.bfloat16),
        'w_out': block_rows([w_attn_out, w_down]).astype(jnp.bfloat16),
        'attn_out_bias': (0.3 * jax.random.normal(shared_keys[10], (D,), jnp.float32)).astype(jnp.bfloat16),
        'mlp_out_bias': (0.3 * jax.random.normal(shared_keys[11], (D,), jnp.float32)).astype(jnp.bfloat16),
    }


def norm_last(features, gain_vec):
    centered = features - jnp.mean(features, axis=-1, keepdims=True)
    variance = jnp.mean(jnp.square(centered), axis=-1, keepdims=True)
    return centered * lax.rsqrt(variance + 1e-6) * gain_vec.astype(jnp.float32)


def reference(tokens, ln_scale, w_in, mlp_bias, q_scale, k_scale, w_out, attn_out_bias, mlp_out_bias):
    out_bias = attn_out_bias.astype(jnp.float32) + mlp_out_bias.astype(jnp.float32)
    unit_bias = mlp_bias.reshape(BLOCKS, FF_BLK).astype(jnp.float32)

    def one_image(image_row):
        tok_f32 = image_row.astype(jnp.float32)
        normed = norm_last(tok_f32, ln_scale).astype(jnp.bfloat16)
        projected = jnp.dot(normed, w_in, preferred_element_type=jnp.float32).astype(jnp.bfloat16)
        projected = projected.reshape(SEQ, BLOCKS, IN_BLK)
        head_shape = (SEQ, HEADS, HEAD)
        queries = norm_last(projected[:, :, :QKV_BLK].reshape(head_shape).astype(jnp.float32), q_scale).astype(jnp.bfloat16)
        keys_n = norm_last(projected[:, :, QKV_BLK:2 * QKV_BLK].reshape(head_shape).astype(jnp.float32), k_scale).astype(jnp.bfloat16)
        values = projected[:, :, 2 * QKV_BLK:3 * QKV_BLK].reshape(head_shape)
        logits = jnp.einsum('qhd,khd->hqk', queries.astype(jnp.float32), keys_n.astype(jnp.float32)) * HEAD ** -0.5
        attn_prob = jax.nn.softmax(logits, axis=-1).astype(jnp.bfloat16)
        mixed = jnp.einsum('hqk,khd->qhd', attn_prob.astype(jnp.float32), values.astype(jnp.float32)).astype(jnp.bfloat16)
        mlp_act = jax.nn.gelu(projected[:, :, 3 * QKV_BLK:].astype(jnp.float32) + unit_bias, approximate=False).astype(jnp.bfloat16)
        joined = jnp.concatenate([mixed.reshape(SEQ, BLOCKS, QKV_BLK), mlp_act], axis=2).reshape(SEQ, -1)
        out_f32 = jnp.dot(joined, w_out, preferred_element_type=jnp.float32)
        return (out_f32 + out_bias + tok_f32).astype(jnp.bfloat16)

    return lax.map(one_image, tokens)
```

```python
import jax
import jax.numpy as jnp
from jax import lax
from jax.experimental import pallas as pl
from jax.experimental.pallas import tpu as pltpu
from jax.sharding import PartitionSpec as P

MESH = pl.DeviceIdType.MESH
F32 = jnp.float32
BF16 = jnp.bfloat16

SEQ = 256
DL = 1280
DTOT = 5120
HD = 128
QKV_W = 1280
HALF_H = 5
FFB = 5120
CW = 512
NJ = FFB // CW
UR = 32
GROUPS = ((0, 128), (128, 96), (224, 32))

NQ = 3 * HALF_H * 2
NA = HALF_H * 2
NM = NJ * (SEQ // UR)
NU = NQ + NA + NM
HOP = 5
A0 = 48

FAR, NEAR, MLP = 0, NQ, 2 * NQ
EARLY = 2 * NQ + NM
LATE = EARLY + NU
NBUF = LATE + NU

P_LN, P_OB, P_QK = NJ, NJ + 3, NJ + 6


def head_norm(feat, gain):
    feat = feat.astype(F32)
    cent = feat - jnp.mean(feat, axis=-1, keepdims=True)
    var = jnp.mean(jnp.square(cent), axis=-1, keepdims=True)
    return (cent * lax.rsqrt(var + 1e-6) * gain).astype(BF16)


def layer_kernel(tok, win, wout, prm, out, buf, wi, wo, xv, zv, acc, att, qkv, act, mxb, stat,
                 wsem, xsem, ssem, rsem, tsend, trecv, msend, mrecv, osem):
    dp = lax.axis_index("dp")
    z = lax.axis_index("my")
    mx = lax.axis_index("mx")
    low = z < 2
    k = jnp.where(low, z, 3 - z)
    side = jnp.where(low, 0, 1)
    inner = jnp.where(low, z + 1, z - 1)
    outer = jnp.where(k == 0, inner, jnp.where(low, z - 1, z + 1))
    core_peer = mx + 1 - 2 * (mx % 2)
    y_peer = (mx + 2) % 4
    near = HALF_H * side
    far = HALF_H * (1 - side)

    def win_copy(col, width, idx):
        cols = pl.ds(pl.multiple_of(col, 128), width)
        return pltpu.make_async_copy(win.at[:, cols], wi.at[:, cols], wsem.at[idx])

    def qkv_copy(t, base, idx):
        return win_copy(t * QKV_W + base * HD, HALF_H * HD, idx)

    def up_copy(j):
        return win_copy(3 * QKV_W + j * CW, CW, 6 + j)

    def attn_w_copy():
        return pltpu.make_async_copy(wout.at[pl.ds(0, QKV_W)], wo.at[pl.ds(0, QKV_W)], wsem.at[6 + NJ])

    def down_copy(j):
        rows = pl.ds(pl.multiple_of(QKV_W + j * CW, 128), CW)
        return pltpu.make_async_copy(wout.at[rows], wo.at[rows], wsem.at[7 + NJ + j])

    x_copy = pltpu.make_async_copy(tok.at[0], xv, xsem)
    x_copy.start()
    for t in range(3):
        qkv_copy(t, far, t).start()
    for t in range(3):
        qkv_copy(t, near, 3 + t).start()
    for j in range(NJ):
        up_copy(j).start()
    attn_w_copy().start()
    for j in range(NJ):
        down_copy(j).start()

    barrier = pltpu.get_barrier_semaphore()
    for i in range(1, 4):
        pl.semaphore_signal(barrier, inc=1, device_id=(dp, (z + i) % 4, mx), device_id_type=MESH)
    for peer in (core_peer, y_peer):
        pl.semaphore_signal(barrier, inc=1, device_id=(dp, z, peer), device_id_type=MESH)

    acc[...] = jnp.zeros_like(acc)

    x_copy.wait()
    xf = xv[...].astype(F32)
    mu = jnp.sum(xf, axis=1, keepdims=True) * (1.0 / DL)
    m2 = jnp.sum(jnp.square(xf - mu), axis=1, keepdims=True)
    lane = lax.broadcasted_iota(jnp.int32, (SEQ, 128), 1)
    stat[z] = jnp.where(lane == 0, mu, m2).T[:8]
    pl.semaphore_wait(barrier, 5)

    def stat_copy(i):
        return pltpu.make_async_remote_copy(
            src_ref=stat.at[z], dst_ref=stat.at[z], send_sem=tsend.at[i], recv_sem=trecv.at[z],
            device_id=(dp, (z + i) % 4, mx), device_id_type=MESH)

    for i in (3, 2, 1):
        stat_copy(i).start()
    for t in range(3):
        qkv_copy(t, far, t).wait()
    for i in range(1, 4):
        src = (z + i) % 4
        pltpu.make_async_copy(stat.at[src], stat.at[src], trecv.at[src]).wait()
    means = [stat[i][0:1] for i in range(4)]
    devs = [stat[i][1:2] for i in range(4)]
    mean = (means[0] + means[1] + means[2] + means[3]) * 0.25
    m2_all = devs[0] + devs[1] + devs[2] + devs[3]
    for i in range(4):
        m2_all = m2_all + DL * jnp.square(means[i] - mean)
    inv = lax.rsqrt(m2_all * (1.0 / DTOT) + 1e-6)
    row = lax.broadcasted_iota(jnp.int32, (128, SEQ), 0)
    cols2 = jnp.where(row == 0, mean, inv).T
    ln_gain = jnp.concatenate([prm[P_LN:P_LN + 1, :], prm[P_LN + 1:P_LN + 2, :], prm[P_LN + 2:P_LN + 3, :256]], axis=1)
    zv[...] = ((xv[...].astype(F32) - cols2[:, 0:1]) * cols2[:, 1:2] * ln_gain).astype(BF16)

    def qkv_piece(p, base, first):
        col = (p % 3) * QKV_W + (base + p // 3) * HD
        part = jnp.dot(zv[...], wi[:, pl.ds(pl.multiple_of(col, 128), HD)], preferred_element_type=F32).astype(BF16)
        for half in range(2):
            for i in range(4):
                r0 = half * 128 + UR * i
                buf[first + 2 * p + half, :, HD * i:HD * (i + 1)] = part[r0:r0 + UR]

    def mlp_chunk(j):
        up_copy(j).wait()
        col = 3 * QKV_W + j * CW
        part = jnp.dot(zv[...], wi[:, pl.ds(pl.multiple_of(col, 128), CW)], preferred_element_type=F32).astype(BF16)
        base = 0
        for r0, rows in GROUPS:
            per = rows // UR
            for i in range(per):
                buf[MLP + base + per * j + i] = part[r0 + UR * i:r0 + UR * (i + 1)]
            base += NJ * per

    def unit_copy(src, dst, which, dst_which, u, target):
        return pltpu.make_async_remote_copy(
            src_ref=buf.at[src], dst_ref=buf.at[dst], send_sem=ssem.at[which, u], recv_sem=rsem.at[dst_which, u],
            device_id=(dp, target, mx), device_id_type=MESH)

    def arrival(slot, which, u):
        return pltpu.make_async_copy(buf.at[slot], buf.at[slot], rsem.at[which, u])

    def kind(u):
        is_q = u < NQ
        is_a = jnp.logical_and(u >= A0, u < A0 + NA)
        m = u - NQ - jnp.where(u >= A0 + NA, NA, 0)
        return is_q, is_a, m

    def put_attention(which, u, unit):
        head = (u - A0) // 2
        half = (u - A0) % 2
        for i in range(4):
            r0 = pl.multiple_of(half * 128 + UR * i, UR)
            att[which, pl.ds(r0, UR), pl.ds(pl.multiple_of(head * HD, HD), HD)] = unit[:, HD * i:HD * (i + 1)]

    def activate(m, h, j):
        pre = h.astype(BF16).astype(F32) + prm[pl.ds(j, 1), :]
        return (0.5 * pre * (1.0 + lax.erf(pre * (0.5 ** 0.5)))).astype(BF16)

    def down(g, j):
        r0, rows = GROUPS[g]
        w0 = pl.multiple_of(QKV_W + j * CW, 128)
        for n in range(DL // 256):
            acc[r0:r0 + rows, 256 * n:256 * (n + 1)] += jnp.dot(
                act[0:rows, :], wo[pl.ds(w0, CW), 256 * n:256 * (n + 1)], preferred_element_type=F32)

    def mx_copy(step, g):
        rows = pl.ds(GROUPS[g][0], GROUPS[g][1])
        return pltpu.make_async_remote_copy(
            src_ref=mxb.at[2 * step, rows], dst_ref=mxb.at[2 * step + 1, rows],
            send_sem=msend.at[step, g], recv_sem=mrecv.at[step, g],
            device_id=(dp, z, (core_peer, y_peer)[step]), device_id_type=MESH)

    def out_copy(g):
        rows = pl.ds(GROUPS[g][0], GROUPS[g][1])
        return pltpu.make_async_copy(xv.at[rows], out.at[0, rows], osem.at[g])

    def reduce_a(g):
        r0, rows = GROUPS[g]
        mxb[0, r0:r0 + rows] = acc[r0:r0 + rows].astype(BF16)
        mx_copy(0, g).start()

    def reduce_b(g):
        r0, rows = GROUPS[g]
        mx_copy(0, g).wait()
        mxb[2, r0:r0 + rows] = (mxb[0, r0:r0 + rows].astype(F32) + mxb[1, r0:r0 + rows].astype(F32)).astype(BF16)
        mx_copy(1, g).start()

    def reduce_c(g):
        r0, rows = GROUPS[g]
        mx_copy(1, g).wait()
        total = mxb[2, r0:r0 + rows].astype(F32) + mxb[3, r0:r0 + rows].astype(F32)
        bias = jnp.concatenate([prm[P_OB:P_OB + 1, :], prm[P_OB + 1:P_OB + 2, :], prm[P_OB + 2:P_OB + 3, :256]], axis=1)
        xv[r0:r0 + rows] = (total + bias + xv[r0:r0 + rows].astype(F32)).astype(BF16)
        out_copy(g).start()

    qkv_piece(0, far, FAR)

    late_lag = (3 - k) * HOP
    group_end = []
    done = 0
    for _, rows in GROUPS:
        done += NJ * rows // UR
        group_end.append(NQ + NA + done - 1)

    def step(s, carry):
        @pl.when(s < 14)
        def _():
            qkv_piece(s + 1, far, FAR)

        @pl.when(s == 2)
        def _():
            for t in range(3):
                qkv_copy(t, near, 3 + t).wait()

        @pl.when(jnp.logical_and(s >= 2, s < 17))
        def _():
            qkv_piece(s - 2, near, NEAR)

        @pl.when(jnp.logical_and(s >= 17, s < 17 + NJ))
        def _():
            mlp_chunk(s - 17)

        ue = s - k * HOP

        @pl.when(jnp.logical_and(ue >= 0, ue < NU))
        def _():
            is_q, is_a, m = kind(ue)
            own = jnp.where(is_q, FAR + ue, MLP + m)
            slot = EARLY + ue

            @pl.when(k == 1)
            def _():
                arrival(slot, 0, ue).wait()

                @pl.when(jnp.logical_not(is_a))
                def _():
                    buf[slot] = (buf[slot].astype(F32) + buf[own].astype(F32)).astype(BF16)

            src = jnp.where(jnp.logical_or(k == 1, is_a), slot, own)
            unit_copy(src, jnp.where(k == 0, EARLY, LATE) + ue, 0, k, ue, inner).start()

            @pl.when(jnp.logical_and(k == 1, is_a))
            def _():
                put_attention(0, ue, buf[slot])

        ul = s - late_lag

        @pl.when(jnp.logical_and(ul >= 0, ul < NU))
        def _():
            is_q, is_a, m = kind(ul)
            own = jnp.where(is_q, NEAR + ul, MLP + m)
            slot = LATE + ul
            arrival(slot, 1, ul).wait()
            is_m = jnp.logical_not(jnp.logical_or(is_q, is_a))
            g = jnp.where(m < 40, 0, jnp.where(m < 70, 1, 2))
            per = jnp.where(g == 0, 4, jnp.where(g == 1, 3, 1))
            mm = m - jnp.where(g == 0, 0, jnp.where(g == 1, 40, 70))
            j = jnp.where(g == 0, mm // 4, jnp.where(g == 1, mm // 3, mm))
            i = mm - per * j

            @pl.when(is_m)
            def _():
                other = jnp.where(k == 0, own, EARLY + ul)
                h = buf[slot].astype(F32) + buf[other].astype(F32)
                act[pl.ds(pl.multiple_of(i * UR, UR), UR), :] = activate(m, h, j)

            @pl.when(k == 1)
            def _():
                @pl.when(jnp.logical_not(is_a))
                def _():
                    buf[slot] = (buf[slot].astype(F32) + buf[own].astype(F32)).astype(BF16)

                unit_copy(slot, slot, 1, 1, ul, outer).start()

            @pl.when(is_a)
            def _():
                put_attention(1, ul, buf[slot])

            @pl.when(jnp.logical_and(k == 0, is_q))
            def _():
                whole = (buf[slot].astype(F32) + buf[own].astype(F32)).astype(BF16)
                p = ul // 2
                half = ul % 2
                for q in range(4):
                    r0 = pl.multiple_of(half * 128 + UR * q, UR)
                    qkv[p, pl.ds(r0, UR), :] = whole[:, HD * q:HD * (q + 1)]

            for gg in range(3):
                @pl.when(jnp.logical_and(is_m, jnp.logical_and(g == gg, i == per - 1)))
                def _():
                    if gg == 0:
                        down_copy(j).wait()
                    down(gg, j)

            for gg in range(3):
                @pl.when(ul == group_end[gg])
                def _():
                    reduce_a(gg)

            for gg in range(2):
                @pl.when(ul == group_end[gg] + 4)
                def _():
                    reduce_b(gg)

            @pl.when(ul == group_end[0] + 18)
            def _():
                reduce_c(0)

        head = (ul + 1) // 6 - 1

        @pl.when(jnp.logical_and(jnp.logical_and(k == 0, ul < NQ), jnp.logical_and(ul >= 5, (ul + 1) % 6 == 0)))
        def _():
            query = head_norm(qkv[3 * head], prm[P_QK:P_QK + 1, 0:HD])
            key = head_norm(qkv[3 * head + 1], prm[P_QK:P_QK + 1, HD:2 * HD])
            logits = lax.dot_general(query, key, (((1,), (1,)), ((), ())), preferred_element_type=F32) * (HD ** -0.5)
            expo = jnp.exp(logits - jnp.max(logits, axis=-1, keepdims=True))
            prob = (expo / jnp.sum(expo, axis=-1, keepdims=True)).astype(BF16)
            mixed = jnp.dot(prob, qkv[3 * head + 2], preferred_element_type=F32).astype(BF16)
            att[0, :, pl.ds(pl.multiple_of(head * HD, HD), HD)] = mixed
            for half in range(2):
                for q in range(4):
                    r0 = half * 128 + UR * q
                    buf[EARLY + A0 + 2 * head + half, :, HD * q:HD * (q + 1)] = mixed[r0:r0 + UR]

        n = ul - (A0 + NA)

        @pl.when(n == 0)
        def _():
            attn_w_copy().wait()

        @pl.when(jnp.logical_and(n >= 0, n < DL // 256))
        def _():
            cols = pl.ds(pl.multiple_of(n * 256, 256), 256)
            near_rows = pl.ds(pl.multiple_of(near * HD, HD), HALF_H * HD)
            far_rows = pl.ds(pl.multiple_of(far * HD, HD), HALF_H * HD)
            acc[:, cols] += (jnp.dot(att[0], wo[near_rows, cols], preferred_element_type=F32)
                             + jnp.dot(att[1], wo[far_rows, cols], preferred_element_type=F32))

        return carry

    lax.fori_loop(0, NU + late_lag, step, 0)
    reduce_c(1)
    reduce_b(2)

    def drain(u, carry):
        unit_copy(0, 0, 0, 0, u, inner).wait_send()

        @pl.when(k == 1)
        def _():
            unit_copy(0, 0, 1, 1, u, outer).wait_send()

        return carry

    lax.fori_loop(0, NU, drain, 0)
    for i in range(1, 4):
        stat_copy(i).wait_send()
    reduce_c(2)
    for g in range(3):
        out_copy(g).wait()


def solution(mesh):
    def local_layer(tokens, ln_scale, w_in, mlp_bias, q_scale, k_scale, w_out, attn_out_bias, mlp_out_bias):
        pad = jnp.zeros((256,), F32)
        table = jnp.concatenate([
            mlp_bias.astype(F32), ln_scale.astype(F32), pad,
            attn_out_bias.astype(F32) + mlp_out_bias.astype(F32), pad,
            q_scale.astype(F32), k_scale.astype(F32), pad]).reshape(-1, CW)
        dma = pltpu.SemaphoreType.DMA
        anyspace = pl.BlockSpec(memory_space=pl.ANY)
        return pl.pallas_call(
            layer_kernel,
            out_shape=jax.ShapeDtypeStruct((1, SEQ, DL), BF16),
            in_specs=[anyspace, anyspace, anyspace, pl.BlockSpec(memory_space=pltpu.VMEM)],
            out_specs=anyspace,
            scratch_shapes=[
                pltpu.VMEM((NBUF, UR, CW), BF16),
                pltpu.VMEM((DL, 3 * QKV_W + FFB), BF16),
                pltpu.VMEM((QKV_W + FFB, DL), BF16),
                pltpu.VMEM((SEQ, DL), BF16),
                pltpu.VMEM((SEQ, DL), BF16),
                pltpu.VMEM((SEQ, DL), F32),
                pltpu.VMEM((2, SEQ, HALF_H * HD), BF16),
                pltpu.VMEM((3 * HALF_H, SEQ, HD), BF16),
                pltpu.VMEM((128, CW), BF16),
                pltpu.VMEM((4, SEQ, DL), BF16),
                pltpu.VMEM((4, 8, SEQ), F32),
                dma((7 + 2 * NJ,)),
                dma,
                dma((2, NU)),
                dma((2, NU)),
                dma((4,)),
                dma((4,)),
                dma((2, 3)),
                dma((2, 3)),
                dma((3,)),
            ],
            compiler_params=pltpu.CompilerParams(
                collective_id=0, has_side_effects=True, vmem_limit_bytes=67043328),
            name="layer",
        )(tokens, w_in, w_out, table)

    specs_in = (P('dp', None, 'my'), P('my'), P('my', 'mx'), P('mx'), P(), P(), P('mx', 'my'), P('my'), P('my'))
    return jax.shard_map(local_layer, mesh=mesh, in_specs=specs_in, out_specs=P('dp', None, 'my'), check_vma=False)
```

```python
import jax
import jax.numpy as jnp
from jax import lax
from jax.experimental import pallas as pl
from jax.experimental.pallas import tpu as pltpu
from jax.sharding import PartitionSpec as P

MESH = pl.DeviceIdType.MESH
F32 = jnp.float32
BF16 = jnp.bfloat16

SEQ = 256
DL = 1280
DTOT = 5120
HD = 128
QKV_W = 1280
HALF_H = 5
SIDE_W = HALF_H * HD
FFB = 5120
CW = 512
NJ = FFB // CW
UR = 64
GROUPS = ((0, 128, 0), (128, 64, 20), (192, 32, 30), (224, 32, 35))
NG = len(GROUPS)

NQ = 3 * HALF_H
NA = HALF_H
NM = 40
NU = NQ + NA + NM
HOP = 3
A0 = 24
GROUP_END = (39, 49, 54, 59)

FAR, NEAR, MLP = 0, NQ, 2 * NQ
EARLY = 2 * NQ + NM
LATE = EARLY + NU
NBUF = LATE + NU
BLOCKS = tuple((t, c, w) for t in range(3) for c, w in ((0, 256), (256, 256), (512, 128)))


def head_norm(feat, gain):
    feat = feat.astype(F32)
    cent = feat - jnp.mean(feat, axis=-1, keepdims=True)
    var = jnp.mean(jnp.square(cent), axis=-1, keepdims=True)
    return (cent * lax.rsqrt(var + 1e-6) * gain).astype(BF16)


def both(*conds):
    out = conds[0]
    for cond in conds[1:]:
        out = jnp.logical_and(out, cond)
    return out


def layer_kernel(tok, lng, win, mb, qs, ks, wout, ab, ob, out, buf, wi, wo, xv, zv, acc, att, qkv, act, mxb, stat,
                 lng_v, mb_v, qs_v, ks_v, ab_v, ob_v, bias_v,
                 wsem, xsem, psem, ssem, rsem, tsend, trecv, msend, mrecv, osem):
    dp = lax.axis_index("dp")
    z = lax.axis_index("my")
    mx = lax.axis_index("mx")
    low = z < 2
    k = jnp.where(low, z, 3 - z)
    side = jnp.where(low, 0, 1)
    inner = jnp.where(low, z + 1, z - 1)
    outer = jnp.where(k == 0, inner, jnp.where(low, z - 1, z + 1))
    core_peer = mx + 1 - 2 * (mx % 2)
    y_peer = (mx + 2) % 4
    near = SIDE_W * side
    far = SIDE_W * (1 - side)

    def win_copy(col, width, idx):
        cols = pl.ds(pl.multiple_of(col, 128), width)
        return pltpu.make_async_copy(win.at[:, cols], wi.at[:, cols], wsem.at[idx])

    def qkv_copy(t, base, idx):
        return win_copy(t * QKV_W + base, SIDE_W, idx)

    def up_copy(j):
        return win_copy(3 * QKV_W + j * CW, CW, 6 + j)

    def attn_w_copy():
        return pltpu.make_async_copy(wout.at[pl.ds(0, QKV_W)], wo.at[pl.ds(0, QKV_W)], wsem.at[6 + NJ])

    def down_copy(j):
        rows = pl.ds(pl.multiple_of(QKV_W + j * CW, 128), CW)
        return pltpu.make_async_copy(wout.at[rows], wo.at[rows], wsem.at[7 + NJ + j])

    x_copy = pltpu.make_async_copy(tok.at[0], xv, xsem)
    x_copy.start()
    small = [pltpu.make_async_copy(a, b, psem.at[i]) for i, (a, b) in enumerate(
        ((lng, lng_v), (mb, mb_v), (qs, qs_v), (ks, ks_v), (ab, ab_v), (ob, ob_v)))]
    for copy in small:
        copy.start()

    barrier = pltpu.get_barrier_semaphore()
    for i in (3, 2, 1):
        pl.semaphore_signal(barrier, inc=1, device_id=(dp, (z + i) % 4, mx), device_id_type=MESH)
    for peer in (core_peer, y_peer):
        pl.semaphore_signal(barrier, inc=1, device_id=(dp, z, peer), device_id_type=MESH)

    for t in range(3):
        qkv_copy(t, far, t).start()

    x_copy.wait()
    xf = xv[...].astype(F32)
    mu = jnp.sum(xf, axis=1, keepdims=True) * (1.0 / DL)
    m2 = jnp.sum(jnp.square(xf - mu), axis=1, keepdims=True)
    lane = lax.broadcasted_iota(jnp.int32, (SEQ, 128), 1)
    stat[z] = jnp.where(lane == 0, mu, m2).T[:8]
    pl.semaphore_wait(barrier, 5)

    def stat_copy(i):
        return pltpu.make_async_remote_copy(
            src_ref=stat.at[z], dst_ref=stat.at[z], send_sem=tsend.at[i], recv_sem=trecv.at[z],
            device_id=(dp, (z + i) % 4, mx), device_id_type=MESH)

    for i in (3, 2, 1):
        stat_copy(i).start()
    acc[...] = jnp.zeros_like(acc)
    for copy in small:
        copy.wait()
    bias_v[...] = mb_v[...].astype(F32).reshape(NJ, CW)
    ln_gain = lng_v[...].astype(F32).reshape(1, DL)
    for t in range(3):
        qkv_copy(t, far, t).wait()
    for i in range(1, 4):
        src = (z + i) % 4
        pltpu.make_async_copy(stat.at[src], stat.at[src], trecv.at[src]).wait()
    for t in range(3):
        qkv_copy(t, near, 3 + t).start()
    means = [stat[i][0:1] for i in range(4)]
    devs = [stat[i][1:2] for i in range(4)]
    mean = (means[0] + means[1] + means[2] + means[3]) * 0.25
    m2_all = devs[0] + devs[1] + devs[2] + devs[3]
    for i in range(4):
        m2_all = m2_all + DL * jnp.square(means[i] - mean)
    inv = lax.rsqrt(m2_all * (1.0 / DTOT) + 1e-6)
    row = lax.broadcasted_iota(jnp.int32, (128, SEQ), 0)
    cols2 = jnp.where(row == 0, mean, inv).T
    zv[...] = ((xv[...].astype(F32) - cols2[:, 0:1]) * cols2[:, 1:2] * ln_gain).astype(BF16)

    def qkv_block(b, base, first):
        t, c, width = BLOCKS[b]
        cols = pl.ds(pl.multiple_of(t * QKV_W + base + c, 128), width)
        part = jnp.dot(zv[...], wi[:, cols], preferred_element_type=F32).astype(BF16)
        for h in range(width // HD):
            for i in range(4):
                buf[first + HALF_H * t + c // HD + h, :, HD * i:HD * (i + 1)] = part[
                    UR * i:UR * (i + 1), HD * h:HD * (h + 1)]

    def mlp_chunk(j):
        up_copy(j).wait()
        cols = pl.ds(pl.multiple_of(3 * QKV_W + j * CW, 128), CW)
        part = jnp.dot(zv[...], wi[:, cols], preferred_element_type=F32).astype(BF16)
        buf[MLP + 2 * j] = part[0:64]
        buf[MLP + 2 * j + 1] = part[64:128]
        buf[MLP + 20 + j] = part[128:192]
        rows = pl.ds(pl.multiple_of(32 * (j % 2), 32), 32)
        buf[MLP + 30 + j // 2, rows] = part[192:224]
        buf[MLP + 35 + j // 2, rows] = part[224:256]

    def unit_copy(src, dst, which, dst_which, u, target):
        return pltpu.make_async_remote_copy(
            src_ref=buf.at[src], dst_ref=buf.at[dst], send_sem=ssem.at[which, u], recv_sem=rsem.at[dst_which, u],
            device_id=(dp, target, mx), device_id_type=MESH)

    def arrival(slot, which, u):
        return pltpu.make_async_copy(buf.at[slot], buf.at[slot], rsem.at[which, u])

    def kind(u):
        is_q = u < NQ
        is_a = both(u >= A0, u < A0 + NA)
        m = u - NQ - jnp.where(u >= A0 + NA, NA, 0)
        return is_q, is_a, m

    def put_attention(which, u, unit):
        cols = pl.ds(pl.multiple_of((u - A0) * HD, HD), HD)
        for i in range(4):
            att[which, UR * i:UR * (i + 1), cols] = unit[:, HD * i:HD * (i + 1)]

    def activate(h, j):
        pre = h.astype(BF16).astype(F32) + bias_v[pl.ds(j, 1), :]
        return (0.5 * pre * (1.0 + lax.erf(pre * (0.5 ** 0.5)))).astype(BF16)

    def down(g, first_row, j):
        r0, rows, _ = GROUPS[g]
        w0 = pl.multiple_of(QKV_W + j * CW, 128)
        for n in range(DL // 256):
            acc[r0:r0 + rows, 256 * n:256 * (n + 1)] += jnp.dot(
                act[first_row:first_row + rows, :], wo[pl.ds(w0, CW), 256 * n:256 * (n + 1)],
                preferred_element_type=F32)

    def mx_copy(step, g):
        rows = pl.ds(GROUPS[g][0], GROUPS[g][1])
        return pltpu.make_async_remote_copy(
            src_ref=mxb.at[2 * step, rows], dst_ref=mxb.at[2 * step + 1, rows],
            send_sem=msend.at[step, g], recv_sem=mrecv.at[step, g],
            device_id=(dp, z, (core_peer, y_peer)[step]), device_id_type=MESH)

    def out_copy(g):
        rows = pl.ds(GROUPS[g][0], GROUPS[g][1])
        return pltpu.make_async_copy(xv.at[rows], out.at[0, rows], osem.at[g])

    def reduce_a(g):
        r0, rows, _ = GROUPS[g]
        mxb[0, r0:r0 + rows] = acc[r0:r0 + rows].astype(BF16)
        mx_copy(0, g).start()

    def reduce_b(g):
        r0, rows, _ = GROUPS[g]
        mx_copy(0, g).wait()
        mxb[2, r0:r0 + rows] = (mxb[0, r0:r0 + rows].astype(F32) + mxb[1, r0:r0 + rows].astype(F32)).astype(BF16)
        mx_copy(1, g).start()

    def reduce_c(g):
        r0, rows, _ = GROUPS[g]
        bias = (ab_v[...].astype(F32) + ob_v[...].astype(F32)).reshape(1, DL)
        mx_copy(1, g).wait()
        total = mxb[2, r0:r0 + rows].astype(F32) + mxb[3, r0:r0 + rows].astype(F32)
        xv[r0:r0 + rows] = (total + bias + xv[r0:r0 + rows].astype(F32)).astype(BF16)
        out_copy(g).start()

    qkv_block(0, far, FAR)

    late_lag = (3 - k) * HOP
    near_first = 3
    mlp_first = near_first + len(BLOCKS) - 2

    def step(s, carry):
        for b in range(1, len(BLOCKS)):
            @pl.when(s == b - 1)
            def _():
                qkv_block(b, far, FAR)

        @pl.when(both(s >= 1, s < 1 + NJ))
        def _():
            up_copy(s - 1).start()

        @pl.when(s == 12)
        def _():
            attn_w_copy().start()

        @pl.when(both(s >= 14, s < 14 + NJ))
        def _():
            down_copy(s - 14).start()

        ue = s - k * HOP

        @pl.when(both(ue >= 0, ue < NU))
        def _():
            is_q, is_a, m = kind(ue)
            own = jnp.where(is_q, FAR + ue, MLP + m)
            slot = EARLY + ue

            @pl.when(k == 1)
            def _():
                arrival(slot, 0, ue).wait()

                @pl.when(jnp.logical_not(is_a))
                def _():
                    buf[slot] = (buf[slot].astype(F32) + buf[own].astype(F32)).astype(BF16)

            src = jnp.where(jnp.logical_or(k == 1, is_a), slot, own)
            unit_copy(src, jnp.where(k == 0, EARLY, LATE) + ue, 0, k, ue, inner).start()

            @pl.when(both(k == 1, is_a))
            def _():
                put_attention(0, ue, buf[slot])

        for b in range(len(BLOCKS)):
            @pl.when(s == near_first + b)
            def _():
                if b % 3 == 0:
                    qkv_copy(b // 3, near, 3 + b // 3).wait()
                qkv_block(b, near, NEAR)

        @pl.when(both(s >= mlp_first, s < mlp_first + 2 * NJ, (s - mlp_first) % 2 == 0))
        def _():
            mlp_chunk((s - mlp_first) // 2)

        ul = s - late_lag

        @pl.when(both(ul >= 0, ul < NU))
        def _():
            is_q, is_a, m = kind(ul)
            own = jnp.where(is_q, NEAR + ul, MLP + m)
            slot = LATE + ul
            arrival(slot, 1, ul).wait()
            is_m = jnp.logical_not(jnp.logical_or(is_q, is_a))
            g = jnp.where(m < 20, 0, jnp.where(m < 30, 1, jnp.where(m < 35, 2, 3)))
            pair = 2 * (m - jnp.where(g == 2, 30, 35))
            top = jnp.where(g == 0, m // 2, jnp.where(g == 1, m - 20, pair))
            bottom = jnp.where(g < 2, top, pair + 1)
            arow = pl.multiple_of(jnp.where(g == 0, UR * (m % 2), 0), UR)

            @pl.when(is_m)
            def _():
                other = jnp.where(k == 0, own, EARLY + ul)
                h = buf[slot].astype(F32) + buf[other].astype(F32)
                act[pl.ds(arow, UR), :] = jnp.concatenate(
                    [activate(h[0:32], top), activate(h[32:64], bottom)], axis=0)

            @pl.when(k == 1)
            def _():
                @pl.when(jnp.logical_not(is_a))
                def _():
                    buf[slot] = (buf[slot].astype(F32) + buf[own].astype(F32)).astype(BF16)

                unit_copy(slot, slot, 1, 1, ul, outer).start()

            @pl.when(is_a)
            def _():
                put_attention(1, ul, buf[slot])

            @pl.when(both(k == 0, is_q))
            def _():
                whole = (buf[slot].astype(F32) + buf[own].astype(F32)).astype(BF16)
                for q in range(4):
                    qkv[ul, UR * q:UR * (q + 1), :] = whole[:, HD * q:HD * (q + 1)]

            @pl.when(both(is_m, g == 0, m % 2 == 1))
            def _():
                down_copy(top).wait()
                down(0, 0, top)

            @pl.when(both(is_m, g == 1))
            def _():
                down(1, 0, top)

            for gg in (2, 3):
                @pl.when(both(is_m, g == gg))
                def _():
                    down(gg, 0, top)
                    down(gg, 32, bottom)

            for gg in range(NG):
                @pl.when(ul == GROUP_END[gg])
                def _():
                    reduce_a(gg)

            for gg in range(NG - 1):
                @pl.when(ul == GROUP_END[gg] + 2)
                def _():
                    reduce_b(gg)

            @pl.when(ul == GROUP_END[0] + 9)
            def _():
                reduce_c(0)

            @pl.when(ul == GROUP_END[1] + 7)
            def _():
                reduce_c(1)

        head = ul - 2 * HALF_H

        @pl.when(both(k == 0, head >= 0, head < HALF_H))
        def _():
            query = head_norm(qkv[head], qs_v[...].astype(F32).reshape(1, HD))
            key = head_norm(qkv[HALF_H + head], ks_v[...].astype(F32).reshape(1, HD))
            logits = lax.dot_general(query, key, (((1,), (1,)), ((), ())), preferred_element_type=F32) * (HD ** -0.5)
            expo = jnp.exp(logits - jnp.max(logits, axis=-1, keepdims=True))
            prob = (expo / jnp.sum(expo, axis=-1, keepdims=True)).astype(BF16)
            mixed = jnp.dot(prob, qkv[2 * HALF_H + head], preferred_element_type=F32).astype(BF16)
            att[0, :, pl.ds(pl.multiple_of(head * HD, HD), HD)] = mixed
            for q in range(4):
                buf[EARLY + A0 + head, :, HD * q:HD * (q + 1)] = mixed[UR * q:UR * (q + 1)]

        n = ul - (A0 + NA)

        @pl.when(n == 0)
        def _():
            attn_w_copy().wait()

        @pl.when(both(n >= 0, n < DL // 256))
        def _():
            cols = pl.ds(pl.multiple_of(n * 256, 256), 256)
            near_rows = pl.ds(pl.multiple_of(near, HD), SIDE_W)
            far_rows = pl.ds(pl.multiple_of(far, HD), SIDE_W)
            acc[:, cols] += (jnp.dot(att[0], wo[near_rows, cols], preferred_element_type=F32)
                             + jnp.dot(att[1], wo[far_rows, cols], preferred_element_type=F32))

        return carry

    lax.fori_loop(0, NU + late_lag, step, 0)
    reduce_b(3)
    reduce_c(2)

    def drain(u, carry):
        unit_copy(0, 0, 0, 0, u, inner).wait_send()

        @pl.when(k == 1)
        def _():
            unit_copy(0, 0, 1, 1, u, outer).wait_send()

        return carry

    lax.fori_loop(0, NU, drain, 0)
    for i in range(1, 4):
        stat_copy(i).wait_send()
    reduce_c(3)
    for g in range(NG):
        out_copy(g).wait()


def solution(mesh):
    def local_layer(tokens, ln_scale, w_in, mlp_bias, q_scale, k_scale, w_out, attn_out_bias, mlp_out_bias):
        dma = pltpu.SemaphoreType.DMA
        vmem = pltpu.VMEM
        return pl.pallas_call(
            layer_kernel,
            out_shape=jax.ShapeDtypeStruct((1, SEQ, DL), BF16),
            in_specs=[pl.BlockSpec(memory_space=pl.ANY)] * 9,
            out_specs=pl.BlockSpec(memory_space=pl.ANY),
            scratch_shapes=[
                vmem((NBUF, UR, CW), BF16),
                vmem((DL, 3 * QKV_W + FFB), BF16),
                vmem((QKV_W + FFB, DL), BF16),
                vmem((SEQ, DL), BF16),
                vmem((SEQ, DL), BF16),
                vmem((SEQ, DL), F32),
                vmem((2, SEQ, SIDE_W), BF16),
                vmem((3 * HALF_H, SEQ, HD), BF16),
                vmem((128, CW), BF16),
                vmem((4, SEQ, DL), BF16),
                vmem((4, 8, SEQ), F32),
                vmem((DL,), BF16),
                vmem((FFB,), BF16),
                vmem((HD,), BF16),
                vmem((HD,), BF16),
                vmem((DL,), BF16),
                vmem((DL,), BF16),
                vmem((NJ, CW), F32),
                dma((7 + 2 * NJ,)),
                dma,
                dma((6,)),
                dma((2, NU)),
                dma((2, NU)),
                dma((4,)),
                dma((4,)),
                dma((2, NG)),
                dma((2, NG)),
                dma((NG,)),
            ],
            compiler_params=pltpu.CompilerParams(
                collective_id=0, has_side_effects=True, vmem_limit_bytes=67043328),
            name="layer",
        )(tokens, ln_scale, w_in, mlp_bias, q_scale, k_scale, w_out, attn_out_bias, mlp_out_bias)

    specs_in = (P('dp', None, 'my'), P('my'), P('my', 'mx'), P('mx'), P(), P(), P('mx', 'my'), P('my'), P('my'))
    return jax.shard_map(local_layer, mesh=mesh, in_specs=specs_in, out_specs=P('dp', None, 'my'), check_vma=False)
```
